256 devices in a mesh: group: 4 (over x), seq: 8 (over z_hi, y), expert: 8 (over z_lo, core).
Axes of the slice: x: 4, y: 4, z: 8 (z_hi: 2, z_lo: 4; z = z_hi * 4 + z_lo), core: 2. Of those that a mesh axis runs over, the one named last changes fastest.
Arguments:
- queries: bfloat16 [32, 32, 128], P('expert', 'group')
- keys: bfloat16 [32, 1024, 8, 128], P('expert', 'seq', 'group')
- values: bfloat16 [32, 1024, 8, 128], P('expert', 'seq', 'group'), may hold values from -48 to 48
- block_of_slot: int32 [32, 64], P('expert', 'seq'), may hold values from 0 to 63, each once within a row
- lengths: int32 [32], P('expert'), may hold values from 512 to 1024
- out_proj: bfloat16 [4096, 4096], P('group', 'seq'), may hold values from -0.09375 to 0.09375
- residual: bfloat16 [32, 4096], P('expert', 'seq'), may hold values from -6 to 6
- norm_gain: bfloat16 [4096], replicated, may hold values from 0.25 to 1.75
- router: bfloat16 [4096, 8], replicated, may hold values from -0.09375 to 0.09375
- routes: int32 [32, 2], P('expert'), may hold values from 0 to 7, all different within a row; in each aligned block of 4 rows (0 to 3, 4 to 7, ...) at most 2 rows name the same one
- w_gate: bfloat16 [8, 4096, 14336], P('expert', None, ('group', 'seq')), may hold values from -0.09375 to 0.09375
- w_up: bfloat16 [8, 4096, 14336], P('expert', None, ('group', 'seq')), may hold values from -0.09375 to 0.09375
- w_down: bfloat16 [8, 14336, 4096], P('expert', ('group', 'seq')), may hold values from -0.046875 to 0.046875
Outputs:
- layer_out: bfloat16 [32, 4096], P('expert', 'seq')
The draws below stay inside these ranges and needn't reach their ends.
Inputs may be any that keep to these rules, and one draw needn't show every extreme that they name: `block_of_slot`: each row lists every logical block once. `routes`: the two ids of a row differ; among the 4 rows of one device no expert is named more than 2 times, and in some such blocks one expert is named exactly 2 times.
All inputs are finite; a program needn't handle non-finite values.
Results may differ from the reference program's by a relative error of at most 0.013.
Values may be sent and summed in bfloat16 or wider, within the bound.
A program may use at most 64 MiB of HBM per device.

```python
import math
import jax
import jax.numpy as jnp
import numpy as np
from jax import lax

D = 4096
FF = 14336
HEADS = 32
KV_HEADS = 8
HEAD_DIM = 128
EXPERTS = 8
TOPK = 2
BLOCK = 16
REQ_DEV = 4
CAPACITY = 2
REQUESTS = 32
CONTEXT = 1024
SLOTS = 64


def shared_keys(key):
    return jax.random.normal(jax.random.fold_in(key, 11), (REQUESTS, CONTEXT, KV_HEADS, HEAD_DIM), jnp.float32)


def draw_keys(key, part):
    base = shared_keys(key)
    return base.astype(jnp.bfloat16)


def draw_queries(key, part):
    base = jax.random.normal(jax.random.fold_in(key, 22), (REQUESTS, HEADS, HEAD_DIM), jnp.float32)
    return base.astype(jnp.bfloat16)


def touch_ends(array, stream_key, smallest, high):
    spot = [jax.random.randint(jax.random.fold_in(stream_key, axis), (), 0, length) for axis, length in enumerate(array.shape)]
    longest = array.shape.index(max(array.shape))
    neighbour = spot[:longest] + [(spot[longest] + 1) % array.shape[longest]] + spot[longest + 1:]
    return array.at[tuple(spot)].set(smallest).at[tuple(neighbour)].set(high)


def levels(own_key, dims, shards, smallest, largest):
    def one(dim, parts):
        steps = jax.random.uniform(jax.random.fold_in(jax.random.fold_in(own_key, 6), dim), (parts,), jnp.float32, smallest / len(shards), largest / len(shards))
        return jnp.repeat(jnp.exp(steps), dims[dim] // parts).reshape((-1,) + (1,) * (len(dims) - dim - 1))

    level = one(*shards[0])
    for cut in shards[1:]:
        level = level * one(*cut)
    return level


def routed_block(own_key, own, number, rows, count, top, bound, skew):
    ranking = jax.random.permutation(own_key, count)
    heavy_load, common = shares(count, rows * top, bound, skew, True), shares(count, rows * top, bound, skew, False)
    places = jnp.arange(count)

    def named(sizes, rotation):
        used = int((sizes > 0).sum())
        fixed = max(1, used // 4)
        passed = fixed + (places - fixed + rotation * (used - fixed)) % max(1, count - fixed)
        return jnp.zeros((count,), jnp.int32).at[ranking[jnp.where(places < fixed, places, passed)]].set(jnp.asarray(sizes, jnp.int32))

    sizes = jnp.where(number % 4 == 0, named(heavy_load, number // 4), named(common, number - number // 4 - 1))
    mixed = jax.random.permutation(jax.random.fold_in(own, 3), count)
    source_of, receiver = mixed[0:count // 2 * 2:2], mixed[1:count // 2 * 2:2]
    slack = jnp.minimum(sizes[source_of] - 1, bound - sizes[receiver]) // 2
    slack = jnp.where((source_of == ranking[0]) | (receiver == ranking[0]) | (sizes[receiver] == 0), 0, jnp.maximum(slack, 0))
    passed = jax.random.randint(jax.random.fold_in(own, 4), (count // 2,), 0, 1 << 20) % (slack + 1)
    sizes = sizes.at[source_of].add(-passed).at[receiver].add(passed)
    labels = jnp.searchsorted(jnp.cumsum(sizes), jnp.arange(rows * top), side="right").astype(jnp.int32)
    listing = labels.reshape(top, rows).T
    listing = listing[jax.random.permutation(jax.random.fold_in(own, 1), rows)]
    rotation = jax.random.randint(jax.random.fold_in(own, 2), (rows, 1), 0, top)
    return jnp.take_along_axis(listing, (jnp.arange(top)[None, :] + rotation) % top, axis=1)


def shares(amount, total, limit, lean, full):
    weights = [(1 << 20) // math.isqrt(rank ** lean) + 1 for rank in range(1, amount + 1)]
    largest = limit if full else min(limit, max(-(-total // amount), total * weights[0] // sum(weights)))
    least = 1 if total - largest >= amount - 1 else 0
    given, rest = [largest] + [least] * (amount - 1), total - largest - least * (amount - 1)
    while rest > 0:
        candidates = [i for i in range(1, amount) if given[i] < largest] or [i for i in range(1, amount) if given[i] < limit]
        pool, remaining = sum([weights[i] for i in candidates]), rest
        for i in candidates:
            extra = min(limit - given[i], max(1, remaining * weights[i] // pool), rest)
            given[i] = given[i] + extra
            rest = rest - extra
    return np.array(given)


def noise(stream_key, extent, scale, limit, split=(), kind=jnp.bfloat16):
    array = scale * jax.random.normal(stream_key, extent, jnp.float32)
    if split:
        array = array * levels(stream_key, extent, split, -0.22, 0.18)
    return jnp.clip(array, -limit, limit).astype(kind)


def setup_inputs(seed: int = 0) -> dict:
    arg_keys = jax.random.split(jax.random.key(seed), 14)
    queries = draw_queries(jax.random.fold_in(arg_keys[13], 71), 0)
    keys = draw_keys(jax.random.fold_in(arg_keys[13], 71), 0)
    values = noise(arg_keys[2], (REQUESTS, CONTEXT, KV_HEADS, HEAD_DIM), 8.0, 48.0, ((0, 8), (1, 8), (2, 4)))
    block_of_slot = jax.vmap(lambda own: jax.random.permutation(own, SLOTS))(jax.random.split(arg_keys[3], REQUESTS)).reshape((REQUESTS, SLOTS)).astype(jnp.int32)
    lengths = touch_ends(jax.random.randint(arg_keys[4], (REQUESTS,), CONTEXT // 2, CONTEXT + 1), jax.random.fold_in(arg_keys[4], 1), CONTEXT // 2, CONTEXT).astype(jnp.int32)
    out_proj = noise(arg_keys[5], (HEADS * HEAD_DIM, D), (HEADS * HEAD_DIM) ** -0.5, 0.09375, ((0, 4), (1, 8)))
    residual = noise(arg_keys[6], (REQUESTS, D), 1.0, 6.0, ((0, 8), (1, 8)))
    norm_gain = jnp.clip(1.0 + 0.15 * jax.random.normal(arg_keys[7], (D,), jnp.float32), 0.25, 1.75).astype(jnp.bfloat16)
    router = noise(arg_keys[8], (D, EXPERTS), D ** -0.5, 0.09375)
    routes_keys = jax.random.split(jax.random.fold_in(arg_keys[9], 1), REQUESTS // REQ_DEV)
    routes_turns = jax.random.permutation(jax.random.fold_in(arg_keys[9], 3), REQUESTS // REQ_DEV)
    routes = jax.vmap(lambda own, number: routed_block(jax.random.fold_in(arg_keys[9], 2), own, number, REQ_DEV, EXPERTS, TOPK, CAPACITY, 1))(routes_keys, routes_turns).reshape((REQUESTS, TOPK))
    w_gate = noise(arg_keys[10], (EXPERTS, D, FF), D ** -0.5, 0.09375, ((0, 8), (2, 32)))
    w_up = noise(arg_keys[11], (EXPERTS, D, FF), D ** -0.5, 0.09375, ((0, 8), (2, 32)))
    w_down = noise(arg_keys[12], (EXPERTS, FF, D), FF ** -0.5, 0.046875, ((0, 8), (1, 32)))
    return {"queries": queries, "keys": keys, "values": values, "block_of_slot": block_of_slot, "lengths": lengths, "out_proj": out_proj, "residual": residual, "norm_gain": norm_gain, "router": router, "routes": routes, "w_gate": w_gate, "w_up": w_up, "w_down": w_down}


masked_score = -1e+30

def reference(queries, keys, values, block_of_slot, lengths, out_proj, residual, norm_gain, router, routes, w_gate, w_up, w_down):
    per_kv = HEADS // KV_HEADS
    grouped = queries.astype(jnp.float32).reshape(REQUESTS, KV_HEADS, per_kv, HEAD_DIM)
    scores = jnp.einsum('rkgd,rlkd->rkgl', grouped, keys.astype(jnp.float32), precision=lax.Precision.HIGHEST) * HEAD_DIM ** (-0.5)
    offsets = jnp.arange(BLOCK, dtype=jnp.int32)
    position = (block_of_slot.astype(jnp.int32)[:, :, None] * BLOCK + offsets[None, None, :]).reshape(REQUESTS, CONTEXT)
    visible = (position < lengths.astype(jnp.int32)[:, None])[:, None, None, :]
    masked = jnp.where(visible, scores, masked_score)
    highest = lax.optimization_barrier(jnp.max(masked, axis=-1))
    probs = jnp.where(visible, jnp.exp(masked - highest[..., None]), 0.0)
    totals = lax.optimization_barrier(jnp.sum(probs, axis=-1))
    rounded = lax.optimization_barrier(probs.astype(jnp.bfloat16))
    weighted = jnp.einsum('rkgl,rlkd->rkgd', rounded.astype(jnp.float32), values.astype(jnp.float32), precision=lax.Precision.HIGHEST)
    attended = (weighted / totals[..., None]).astype(jnp.bfloat16).reshape(REQUESTS, HEADS * HEAD_DIM)
    hidden = residual.astype(jnp.float32) + jnp.dot(attended, out_proj, preferred_element_type=jnp.float32)
    meansq = lax.optimization_barrier(jnp.mean(hidden * hidden, axis=-1, keepdims=True))
    normed = (hidden * lax.rsqrt(meansq + 1e-05) * norm_gain.astype(jnp.float32)).astype(jnp.bfloat16)
    logits = jnp.dot(normed, router, preferred_element_type=jnp.float32)
    onehot = (routes.astype(jnp.int32)[:, :, None] == jnp.arange(EXPERTS, dtype=jnp.int32)[None, None, :]).astype(jnp.float32)
    chosen = lax.optimization_barrier(jnp.sum(onehot * logits[:, None, :], axis=-1))
    gate_probs = jax.nn.softmax(chosen, axis=-1)
    mixing = lax.optimization_barrier(jnp.sum(gate_probs[:, :, None] * onehot, axis=1))
    expert_mix = jnp.zeros((REQUESTS, D), jnp.float32)
    for expert in range(EXPERTS):
        gate_act = jnp.dot(normed, w_gate[expert], preferred_element_type=jnp.float32)
        upper = jnp.dot(normed, w_up[expert], preferred_element_type=jnp.float32)
        activated = (jax.nn.silu(gate_act) * upper).astype(jnp.bfloat16)
        expert_out = lax.optimization_barrier(jnp.dot(activated, w_down[expert], preferred_element_type=jnp.float32).astype(jnp.bfloat16))
        expert_mix = expert_mix + mixing[:, expert][:, None] * expert_out.astype(jnp.float32)
    return (hidden + expert_mix).astype(jnp.bfloat16)
```

```python
import jax
import jax.numpy as jnp
from jax import lax
from jax.experimental import pallas as pl
from jax.experimental.pallas import tpu as pltpu
from jax.sharding import PartitionSpec as P

BLOCK = 16
MASKED = -1e30
F32 = jnp.float32
BF16 = jnp.bfloat16
I32 = jnp.int32
NT = (((1,), (1,)), ((), ()))
NN = (((1,), (0,)), ((), ()))


def dot(a, b, dims=NN):
    return lax.dot_general(a, b, dims, preferred_element_type=F32)


def iota(shape, dim):
    return lax.broadcasted_iota(I32, shape, dim)


def kernel(
    blk_s, len_s, rt_s,
    q_h, k_h, v_h, wo_h, res_h, gain_h, rtr_h, wg_h, wu_h, wd_h,
    out_ref,
    q_v, k_v, v_v, wo_v, res_v, gain_v, rtr_v, wg_v, wu_v, wd_v,
    rt_buf, o1, s1, o2, s2, att, r16, b_buf, c_buf, d_buf, u_buf, gate_acc, up_acc,
    e_src, e_buf, g_src, g_buf, f16,
    local_sem, rt_send, rt_recv, a1_send, a1_recv, a2_send, a2_recv, b_send, b_recv,
    c_send, c_recv, d_send, d_recv, e_send, e_recv, g_send, g_recv,
):
    g = lax.axis_index("group")
    s = lax.axis_index("seq")
    e = lax.axis_index("expert")
    zh, y = s // 4, s % 4
    zl, core = e // 2, e % 2
    zc = zh * 8 + e
    xy = g * 4 + y

    def at(gg, ss, ee):
        return {"group": gg, "seq": ss, "expert": ee}

    def remote(src, dst, ssem, rsem, where):
        return pltpu.make_async_remote_copy(
            src_ref=src, dst_ref=dst, send_sem=ssem, recv_sem=rsem,
            device_id=where, device_id_type=pl.DeviceIdType.MESH,
        )

    pairs = [
        (q_h, q_v), (k_h, k_v), (v_h, v_v), (wo_h, wo_v), (res_h, res_v),
        (gain_h, gain_v), (rtr_h, rtr_v), (wg_h, wg_v), (wu_h, wu_v), (wd_h, wd_v),
    ]
    loads = [pltpu.make_async_copy(a, b, local_sem.at[i]) for i, (a, b) in enumerate(pairs)]
    for load in loads:
        load.start()

    barrier = pltpu.get_barrier_semaphore()

    def greet(where):
        pl.semaphore_signal(barrier, inc=1, device_id=where, device_id_type=pl.DeviceIdType.MESH)

    for d in range(1, 16):
        t = (xy + d) % 16
        greet(at(t // 4, zh * 4 + t % 4, e))
    for d in range(1, 16):
        t = (zc + d) % 16
        greet(at(g, (t // 8) * 4 + y, t % 8))
    for t in range(16):
        @pl.when(jnp.logical_not((g == zl) & (zc == t)))
        def _(t=t):
            greet(at(zl, (t // 8) * 4 + y, t % 8))

    row8, lane8 = iota((8, 128), 0), iota((8, 128), 1)
    codes = jnp.full((8, 128), -1, I32)
    count = jnp.zeros((8, 128), I32)
    for tok in range(4):
        first, second = rt_s[0, tok], rt_s[1, tok]
        hit0, hit1 = row8 == first, row8 == second
        hit = hit0 | hit1
        other = jnp.where(hit0, second, first)
        codes = jnp.where((lane8 % 4 == tok) & hit, count + 2 * other, codes)
        count = count + jnp.where(hit, 1, 0)
    rt_buf[e] = codes

    eye = iota((32, 128), 0) == iota((32, 128), 1)
    lane = iota((1, 256), 1)
    parity = iota((8, 256), 1) % 2 == iota((8, 256), 0) // 4
    for i in range(3):
        loads[i].wait()
    outs, maxes, sums = [], [], []
    for r in range(4):
        sc = dot(q_v[r], k_v[r], NT) * (128 ** -0.5)
        limit = jnp.zeros((1, 256), I32)
        for j in range(8):
            limit = jnp.where(lane // 32 == j, len_s[r] - BLOCK * blk_s[r, j], limit)
        live = parity & ((lane // 2) % BLOCK < limit)
        sc = jnp.where(live, sc, MASKED)
        m = jnp.max(sc, axis=1, keepdims=True)
        p = jnp.where(live, jnp.exp(sc - m), 0.0)
        sums.append(jnp.sum(p, axis=1, keepdims=True))
        maxes.append(m)
        outs.append(dot(p.astype(BF16), v_v[r]))

    def to_row(col):
        return jnp.sum(jnp.where(eye, col, 0.0), axis=0, keepdims=True)

    def to_col(row):
        return jnp.sum(jnp.where(eye, row, 0.0), axis=1, keepdims=True)

    o1[y] = jnp.concatenate(outs, axis=0).astype(BF16)
    s1[y, 0:1, :] = to_row(jnp.concatenate(maxes, axis=0))
    s1[y, 1:2, :] = to_row(jnp.concatenate(sums, axis=0))

    self_case = (g == zl).astype(I32)
    pl.semaphore_wait(barrier, 46 - self_case)

    sends = []
    for d in (2, 1, 3):
        to = at(g, zh * 4 + (y + d) % 4, e)
        a = remote(o1.at[y], o1.at[y], a1_send.at[2 * d], a1_recv.at[2 * y], to)
        b = remote(s1.at[y], s1.at[y], a1_send.at[2 * d + 1], a1_recv.at[2 * y + 1], to)
        a.start()
        b.start()
        sends += [a, b]
    for d in range(1, 8):
        to = at(g, s, (e + d) % 8)
        a = remote(rt_buf.at[e], rt_buf.at[e], rt_send.at[d], rt_recv.at[e], to)
        a.start()
        sends.append(a)

    me = at(g, s, e)

    def arrived(dst, rsem, ssem):
        remote(dst, dst, ssem, rsem, me).wait_recv()

    loads[4].wait()
    for j in range(4):
        r16[4 * j : 4 * j + 4, :] = res_v[:, 128 * j : 128 * (j + 1)].astype(F32)
    clane = iota((16, 256), 1)
    crow = iota((16, 256), 0)
    comb = jnp.zeros((16, 256), F32)
    clane_e, clane_blk, clane_rank = (clane // 16) % 8, (clane // 4) % 4, clane % 2
    fits = ((clane // 2) % 2 == core) & (clane_blk == crow // 4)
    ccount = jnp.zeros((16, 256), I32)
    for tok in range(4):
        hit = (clane_e == rt_s[0, tok]) | (clane_e == rt_s[1, tok])
        comb = jnp.where(fits & hit & (crow % 4 == tok) & (ccount == clane_rank), 1.0, comb)
        ccount = ccount + jnp.where(hit, 1, 0)
    comb = comb.astype(BF16)

    for d in (1, 3, 2):
        src = (y + d) % 4
        arrived(o1.at[src], a1_recv.at[2 * src], a1_send.at[0])
        arrived(s1.at[src], a1_recv.at[2 * src + 1], a1_send.at[0])
    ms = [s1[i, 0:1, :] for i in range(4)]
    top = jnp.maximum(jnp.maximum(ms[0], ms[1]), jnp.maximum(ms[2], ms[3]))
    total = jnp.zeros((1, 128), F32)
    merged = jnp.zeros((32, 128), F32)
    for i in range(4):
        w = jnp.exp(ms[i] - top)
        total = total + w * s1[i, 1:2, :]
        merged = merged + to_col(w) * o1[i].astype(F32)
    o2[zh] = merged.astype(BF16)
    s2[zh, 0:1, :] = top
    s2[zh, 1:2, :] = total
    to = at(g, (1 - zh) * 4 + y, e)
    a = remote(o2.at[zh], o2.at[zh], a2_send.at[0], a2_recv.at[0], to)
    b = remote(s2.at[zh], s2.at[zh], a2_send.at[1], a2_recv.at[1], to)
    a.start()
    b.start()
    sends += [a, b]

    for d in range(1, 8):
        src = (e + d) % 8
        arrived(rt_buf.at[src], rt_recv.at[src], rt_send.at[0])
    lane1 = iota((1, 128), 1)
    code = jnp.full((1, 128), -1, I32)
    for i in range(8):
        mine = jnp.sum(jnp.where(row8 == e, rt_buf[i], 0), axis=0, keepdims=True)
        code = jnp.where(lane1 // 16 == i, mine, code)
    rank = jnp.where(code >= 0, code % 2, -1)
    other_lane = jnp.where(code >= 0, code // 2, 0)
    srow, slane = iota((64, 128), 0), iota((64, 128), 1)
    pick = (
        (srow % 2 == rank) & ((srow // 2) % 8 == slane // 16) & (srow // 16 == (slane // 4) % 4)
    )
    select = jnp.where(pick, 1.0, 0.0).astype(BF16)
    other_col = jnp.sum(
        jnp.where(pick[0:16], other_lane.astype(F32), 0.0), axis=1, keepdims=True
    )
    eye16 = iota((16, 128), 0) == iota((16, 128), 1)

    def to_row16(col):
        return jnp.sum(jnp.where(eye16, col, 0.0), axis=0, keepdims=True)[:, 0:16]

    other_row = to_row16(other_col)
    loads[3].wait()

    arrived(o2.at[1 - zh], a2_recv.at[0], a2_send.at[0])
    arrived(s2.at[1 - zh], a2_recv.at[1], a2_send.at[1])
    top = jnp.maximum(s2[0, 0:1, :], s2[1, 0:1, :])
    w0, w1 = jnp.exp(s2[0, 0:1, :] - top), jnp.exp(s2[1, 0:1, :] - top)
    total = w0 * s2[0, 1:2, :] + w1 * s2[1, 1:2, :]
    merged = to_col(w0 / total) * o2[0].astype(F32) + to_col(w1 / total) * o2[1].astype(F32)
    att[0:32, :] = merged
    att[32:64, :] = merged
    part = jnp.zeros((8, 512), F32)
    for h in range(8):
        part = part + dot(att[pl.ds(h, 8, stride=8), :].astype(BF16), wo_v[128 * h : 128 * (h + 1), :])
    low = iota((8, 128), 0) < 4
    for j in range(2):
        b_buf[g, 8 * j : 8 * j + 8, :] = jnp.where(
            low, part[:, 256 * j : 256 * j + 128], part[:, 256 * j + 128 : 256 * j + 256]
        )
    for d in (2, 1, 3):
        a = remote(b_buf.at[g], b_buf.at[g], b_send.at[d], b_recv.at[g], at((g + d) % 4, s, e))
        a.start()
        sends.append(a)
    for d in (1, 3, 2):
        src = (g + d) % 4
        arrived(b_buf.at[src], b_recv.at[src], b_send.at[0])
    hidden = ((b_buf[0] + b_buf[1]) + (b_buf[2] + b_buf[3])) + r16[...]
    c_buf[zc] = hidden.astype(BF16)
    for d in (8, 7, 9, 6, 10, 5, 11, 4, 12, 3, 13, 2, 14, 1, 15):
        t = (zc + d) % 16
        a = remote(
            c_buf.at[zc], c_buf.at[zc], c_send.at[d], c_recv.at[zc],
            at(g, (t // 8) * 4 + y, t % 8),
        )
        a.start()
        sends.append(a)
    for i in range(5, 9):
        loads[i].wait()

    for half in range(2):
        zz = (zh + half) % 2
        for d in range(half == 0, 8):
            src = zz * 8 + (e + d) % 8
            arrived(c_buf.at[src], c_recv.at[src], c_send.at[0])
        rows = c_buf[pl.ds(zz * 8, 8)].reshape(128, 128)
        taken = dot(select, rows).astype(BF16)
        for j in range(4):
            d_buf[y, zz, :, 128 * j : 128 * (j + 1)] = taken[16 * j : 16 * j + 16]
        for d in (2, 1, 3):
            a = remote(
                d_buf.at[y, zz], d_buf.at[y, zz], d_send.at[2 * d + half], d_recv.at[2 * y + zz],
                at(g, zh * 4 + (y + d) % 4, e),
            )
            a.start()
            sends.append(a)

    square = jnp.zeros((16, 1), F32)
    logits = jnp.zeros((8, 16), F32)
    for n, d in enumerate((0, 1, 3, 2)):
        src = (y + d) % 4
        for half in range(2):
            zz = (zh + half) % 2
            if d:
                arrived(d_buf.at[src, zz], d_recv.at[2 * src + zz], d_send.at[0])
            x = d_buf[src, zz].astype(F32)
            square = square + jnp.sum(x * x, axis=1, keepdims=True)
            cols = pl.ds(pl.multiple_of((zz * 4 + src) * 512, 512), 512)
            u = (x * gain_v[0:1, cols].astype(F32)).astype(BF16)
            logits = logits + dot(rtr_v[:, cols], u, NT)
            gg, uu = dot(wg_v[:, cols], u, NT), dot(wu_v[:, cols], u, NT)
            if n == 0 and half == 0:
                gate_acc[...] = gg
                up_acc[...] = uu
            else:
                gate_acc[...] += gg
                up_acc[...] += uu
    scale = to_row16(lax.rsqrt(square * (1.0 / 4096.0) + 1e-05))
    logits = logits * scale
    lrow = iota((8, 16), 0)
    own = jnp.sum(jnp.where(lrow == e, logits, 0.0), axis=0, keepdims=True)
    oth = jnp.sum(jnp.where(lrow.astype(F32) == other_row, logits, 0.0), axis=0, keepdims=True)
    share = 1.0 / (1.0 + jnp.exp(oth - own))
    gate = gate_acc[...] * scale
    act = gate / (1.0 + jnp.exp(-gate)) * (up_acc[...] * (scale * share))
    act = act.T.astype(BF16)
    loads[9].wait()

    for dy in (2, 1, 3, 0):
        ty = (y + dy) % 4
        for zz in range(2):
            cols = pl.ds(pl.multiple_of((zz * 4 + ty) * 512, 512), 512)
            res = dot(act, wd_v[:, cols])
            for tx in range(4):
                tiles = []
                for j in range(2):
                    first = res[8 * (tx // 2) : 8 * (tx // 2) + 8, 256 * j : 256 * j + 128]
                    second = res[8 * (tx // 2) : 8 * (tx // 2) + 8, 256 * j + 128 : 256 * j + 256]
                    if tx % 2:
                        first = pltpu.roll(first, 4, 0)
                    else:
                        second = pltpu.roll(second, 4, 0)
                    tiles.append(jnp.where(low, first, second))
                e_src[tx * 4 + ty, 16 * zz : 16 * zz + 16, :] = jnp.concatenate(tiles, axis=0).astype(BF16)
        for dx in (2, 1, 3, 0):
            if dx or dy:
                t = ((g + dx) % 4) * 4 + ty
                a = remote(
                    e_src.at[t], e_buf.at[xy], e_send.at[4 * dx + dy], e_recv.at[xy],
                    at((g + dx) % 4, zh * 4 + ty, e),
                )
                a.start()
                sends.append(a)
    summed = e_src[xy].astype(F32)
    for dy in (0, 1, 3, 2):
        for dx in (0, 1, 3, 2):
            if dx or dy:
                src = ((g + dx) % 4) * 4 + (y + dy) % 4
                arrived(e_buf.at[src], e_recv.at[src], e_send.at[0])
                summed = summed + e_buf[src].astype(F32)
    for zz in range(2):
        g_src[zz] = summed[16 * zz : 16 * zz + 16].astype(BF16)
    later = []
    for zz in range(2):
        for tx in range(4):
            for cc in range(2):
                ee = g * 2 + cc
                same = (g == tx) & (zh == zz) & (e == ee)
                a = remote(
                    g_src.at[zz], g_buf.at[zc], g_send.at[zz * 8 + tx * 2 + cc], g_recv.at[zc],
                    at(tx, zz * 4 + y, ee),
                )
                pl.when(jnp.logical_not(same))(a.start)
                later.append((same, a))

    @pl.when(g == zl)
    def _():
        g_buf[zc] = g_src[zh]

    for t in range(16):
        @pl.when(jnp.logical_not((g == zl) & (zc == t)))
        def _(t=t):
            arrived(g_buf.at[t], g_recv.at[t], g_send.at[0])
    final = hidden + dot(comb, g_buf[...].reshape(256, 128))
    f16[...] = final
    for j in range(4):
        out_ref[:, 128 * j : 128 * (j + 1)] = f16[4 * j : 4 * j + 4, :].astype(BF16)

    for a in sends:
        a.wait_send()
    for same, a in later:
        pl.when(jnp.logical_not(same))(a.wait_send)


def shards(
    queries, keys, values, block_of_slot, lengths, out_proj, residual, norm_gain, router,
    routes, w_gate, w_up, w_down,
):
    args = (
        block_of_slot, lengths, routes.T,
        queries, keys.reshape(4, 256, 128), values.reshape(4, 256, 128), out_proj, residual,
        norm_gain.reshape(1, 4096), router.T, w_gate[0].T, w_up[0].T, w_down[0],
    )
    smem = pl.BlockSpec(memory_space=pltpu.SMEM)
    hbm = pl.BlockSpec(memory_space=pltpu.HBM)
    dma = pltpu.SemaphoreType.DMA
    vmem = pltpu.VMEM
    return pl.pallas_call(
        kernel,
        out_shape=jax.ShapeDtypeStruct((4, 512), BF16),
        in_specs=[smem] * 3 + [hbm] * 10,
        out_specs=pl.BlockSpec(memory_space=pltpu.VMEM),
        scratch_shapes=[vmem(a.shape, a.dtype) for a in args[3:]]
        + [
            vmem((8, 8, 128), I32),
            vmem((4, 32, 128), BF16), vmem((4, 2, 128), F32),
            vmem((2, 32, 128), BF16), vmem((2, 2, 128), F32),
            vmem((64, 128), F32), vmem((16, 128), F32), vmem((4, 16, 128), F32),
            vmem((16, 16, 128), BF16), vmem((4, 2, 16, 512), BF16), vmem((16, 512), BF16),
            vmem((448, 16), F32), vmem((448, 16), F32),
            vmem((16, 32, 128), BF16), vmem((16, 32, 128), BF16),
            vmem((2, 16, 128), BF16), vmem((16, 16, 128), BF16), vmem((16, 128), F32),
            dma((10,)), dma((8,)), dma((8,)), dma((8,)), dma((8,)), dma((2,)), dma((2,)),
            dma((4,)), dma((4,)), dma((16,)), dma((16,)), dma((8,)), dma((8,)),
            dma((16,)), dma((16,)), dma((16,)), dma((16,)),
        ],
        compiler_params=pltpu.CompilerParams(
            collective_id=0, has_side_effects=True, vmem_limit_bytes=67043328
        ),
    )(*args)


def solution(mesh):
    return jax.shard_map(
        shards,
        mesh=mesh,
        in_specs=(
            P("expert", "group", None),
            P("expert", "seq", "group", None),
            P("expert", "seq", "group", None),
            P("expert", "seq"),
            P("expert"),
            P("group", "seq"),
            P("expert", "seq"),
            P(),
            P(),
            P("expert", None),
            P("expert", None, ("group", "seq")),
            P("expert", None, ("group", "seq")),
            P("expert", ("group", "seq"), None),
        ),
        out_specs=P("expert", "seq"),
        check_vma=False,
    )
```

```python
import jax
import jax.numpy as jnp
from jax import lax
from jax.experimental import pallas as pl
from jax.experimental.pallas import tpu as pltpu
from jax.sharding import PartitionSpec as P

BLOCK = 16
MASKED = -1e30
F32 = jnp.float32
BF16 = jnp.bfloat16
I32 = jnp.int32
NT = (((1,), (1,)), ((), ()))
NN = (((1,), (0,)), ((), ()))


def dot(a, b, dims=NN):
    return lax.dot_general(a, b, dims, preferred_element_type=F32)


def iota(shape, dim):
    return lax.broadcasted_iota(I32, shape, dim)


def kernel(
    blk_h, len_h, rt_h,
    q_h, k_h, v_h, wo_h, res_h, gain_h, rtr_h, wg_h, wu_h, wd_h,
    out_ref,
    blk_s, len_s, rt_s,
    q_v, k_v, v_v, wo_v, res_v, gain_v, rtr_v, wg_v, wu_v, wd_v,
    rt_buf, o1, s1, gain_f, att, r16, b_buf, c_buf, d_buf, u_buf, gate_acc, up_acc,
    e_src, e_buf, g_src, g_buf, f16,
    local_sem, rt_send, rt_recv, a1_send, a1_recv, small_sem, b_send, b_recv,
    c_send, c_recv, d_send, d_recv, e_send, e_recv, g_send, g_recv,
):
    g = lax.axis_index("group")
    s = lax.axis_index("seq")
    e = lax.axis_index("expert")
    zh, y = lax.div(s, 4), lax.rem(s, 4)
    zl, core = lax.div(e, 2), lax.rem(e, 2)
    zc = zh * 8 + e
    xy = g * 4 + y
    oz = 1 - zh
    gs = [g] + [lax.rem(g + d, 4) for d in (1, 2, 3)]
    ys = [y] + [lax.rem(y + d, 4) for d in (1, 2, 3)]
    es = [e] + [lax.rem(e + d, 8) for d in range(1, 8)]
    zs = [zh, oz]
    peers = [zs[d // 4] * 4 + ys[d % 4] for d in range(8)]

    def at(gg, ss, ee):
        return {"group": gg, "seq": ss, "expert": ee}

    def remote(src, dst, ssem, rsem, where):
        return pltpu.make_async_remote_copy(
            src_ref=src, dst_ref=dst, send_sem=ssem, recv_sem=rsem,
            device_id=where, device_id_type=pl.DeviceIdType.MESH,
        )

    barrier = pltpu.get_barrier_semaphore()

    def greet(where):
        pl.semaphore_signal(barrier, inc=1, device_id=where, device_id_type=pl.DeviceIdType.MESH)

    for d in (6, 5, 7, 4, 2, 1, 3):
        greet(at(g, peers[d], e))
    for dz in (1, 0):
        for de in (4, 3, 5, 2, 6, 1, 7):
            greet(at(g, peers[4 * dz], es[de]))
    for d in (2, 1, 3):
        greet(at(gs[d], s, e))

    pairs = [
        (q_h, q_v), (k_h, k_v), (v_h, v_v), (wo_h, wo_v), (res_h, res_v),
        (gain_h, gain_v), (rtr_h, rtr_v), (wg_h, wg_v), (wu_h, wu_v), (wd_h, wd_v),
    ]
    loads = [pltpu.make_async_copy(a, b, local_sem.at[i]) for i, (a, b) in enumerate(pairs)]
    small = [
        pltpu.make_async_copy(a, b, small_sem.at[i])
        for i, (a, b) in enumerate([(rt_h, rt_s), (blk_h, blk_s), (len_h, len_s)])
    ]
    for load in loads[0:3] + small:
        load.start()

    for copy in small:
        copy.wait()
    row8, lane8 = iota((8, 128), 0), iota((8, 128), 1)
    codes = jnp.full((8, 128), -1, I32)
    count = jnp.zeros((8, 128), I32)
    for tok in range(4):
        first, second = rt_s[0, tok], rt_s[1, tok]
        hit0, hit1 = row8 == first, row8 == second
        hit = hit0 | hit1
        other = jnp.where(hit0, second, first)
        codes = jnp.where((lane8 % 4 == tok) & hit, count + 2 * other, codes)
        count = count + jnp.where(hit, 1, 0)
    rt_buf[e] = codes

    eye = iota((32, 128), 0) == iota((32, 128), 1)
    lane = iota((1, 256), 1)
    parity = iota((8, 256), 1) % 2 == iota((8, 256), 0) // 4
    for i in range(3):
        loads[i].wait()
    for load in loads[3:]:
        load.start()
    outs, maxes, sums = [], [], []
    for r in range(4):
        sc = dot(q_v[r], k_v[r], NT) * (128 ** -0.5)
        limit = jnp.zeros((1, 256), I32)
        for j in range(8):
            limit = jnp.where(lane // 32 == j, len_s[r] - BLOCK * blk_s[r, j], limit)
        live = parity & ((lane // 2) % BLOCK < limit)
        sc = jnp.where(live, sc, MASKED)
        m = jnp.max(sc, axis=1, keepdims=True)
        p = jnp.where(live, jnp.exp(sc - m), 0.0)
        sums.append(jnp.sum(p, axis=1, keepdims=True))
        maxes.append(m)
        outs.append(dot(p.astype(BF16), v_v[r]))

    def to_row(col):
        return jnp.sum(jnp.where(eye, col, 0.0), axis=0, keepdims=True)

    def to_col(row):
        return jnp.sum(jnp.where(eye, row, 0.0), axis=1, keepdims=True)

    o1[s] = jnp.concatenate(outs, axis=0).astype(BF16)
    s1[s, 0:1, :] = to_row(jnp.concatenate(maxes, axis=0))
    s1[s, 1:2, :] = to_row(jnp.concatenate(sums, axis=0))

    pl.semaphore_wait(barrier, 24)

    sends = []
    for d in (6, 5, 7, 4, 2, 1, 3):
        to = at(g, peers[d], e)
        a = remote(o1.at[s], o1.at[s], a1_send.at[2 * d], a1_recv.at[2 * s], to)
        b = remote(s1.at[s], s1.at[s], a1_send.at[2 * d + 1], a1_recv.at[2 * s + 1], to)
        a.start()
        b.start()
        sends += [a, b]
    for d in range(1, 8):
        to = at(g, s, es[d])
        a = remote(rt_buf.at[e], rt_buf.at[e], rt_send.at[d], rt_recv.at[e], to)
        a.start()
        sends.append(a)

    me = at(g, s, e)

    def arrived(dst, rsem, ssem):
        remote(dst, dst, ssem, rsem, me).wait_recv()

    loads[4].wait()
    for j in range(4):
        r16[4 * j : 4 * j + 4, :] = res_v[:, 128 * j : 128 * (j + 1)].astype(F32)
    clane = iota((16, 256), 1)
    crow = iota((16, 256), 0)
    comb = jnp.zeros((16, 256), F32)
    clane_e, clane_blk, clane_rank = (clane // 16) % 8, (clane // 4) % 4, clane % 2
    fits = ((clane // 2) % 2 == core) & (clane_blk == crow // 4)
    ccount = jnp.zeros((16, 256), I32)
    for tok in range(4):
        hit = (clane_e == rt_s[0, tok]) | (clane_e == rt_s[1, tok])
        comb = jnp.where(fits & hit & (crow % 4 == tok) & (ccount == clane_rank), 1.0, comb)
        ccount = ccount + jnp.where(hit, 1, 0)
    comb = comb.astype(BF16)

    for d in range(1, 8):
        src = es[d]
        arrived(rt_buf.at[src], rt_recv.at[src], rt_send.at[0])
    lane1 = iota((1, 128), 1)
    code = jnp.full((1, 128), -1, I32)
    for i in range(8):
        mine = jnp.sum(jnp.where(row8 == e, rt_buf[i], 0), axis=0, keepdims=True)
        code = jnp.where(lane1 // 16 == i, mine, code)
    rank = jnp.where(code >= 0, code % 2, -1)
    other_lane = jnp.where(code >= 0, code // 2, 0)
    srow, slane = iota((64, 128), 0), iota((64, 128), 1)
    pick = (
        (srow % 2 == rank) & ((srow // 2) % 8 == slane // 16) & (srow // 16 == (slane // 4) % 4)
    )
    select = jnp.where(pick, 1.0, 0.0).astype(BF16)
    other_col = jnp.sum(
        jnp.where(pick[0:16], other_lane.astype(F32), 0.0), axis=1, keepdims=True
    )
    eye16 = iota((16, 128), 0) == iota((16, 128), 1)

    def to_row16(col):
        return jnp.sum(jnp.where(eye16, col, 0.0), axis=0, keepdims=True)[:, 0:16]

    other_row = to_row16(other_col)
    loads[5].wait()
    gain_f[...] = gain_v[...].astype(F32)
    loads[3].wait()

    for d in (1, 3, 2, 4, 5, 7, 6):
        src = peers[d]
        arrived(o1.at[src], a1_recv.at[2 * src], a1_send.at[0])
        arrived(s1.at[src], a1_recv.at[2 * src + 1], a1_send.at[0])
    ms = [s1[i, 0:1, :] for i in range(8)]
    top = ms[0]
    for m in ms[1:]:
        top = jnp.maximum(top, m)
    ws = [jnp.exp(m - top) for m in ms]
    total = jnp.zeros((1, 128), F32)
    for i in range(8):
        total = total + ws[i] * s1[i, 1:2, :]
    merged = jnp.zeros((32, 128), F32)
    for i in range(8):
        merged = merged + to_col(ws[i] / total) * o1[i].astype(F32)
    att[0:32, :] = merged
    att[32:64, :] = merged
    part = jnp.zeros((8, 512), F32)
    for h in range(8):
        part = part + dot(att[pl.ds(h, 8, stride=8), :].astype(BF16), wo_v[128 * h : 128 * (h + 1), :])
    low = iota((8, 128), 0) < 4
    for j in range(2):
        b_buf[g, 8 * j : 8 * j + 8, :] = jnp.where(
            low, part[:, 256 * j : 256 * j + 128], part[:, 256 * j + 128 : 256 * j + 256]
        )
    for d in (2, 1, 3):
        a = remote(b_buf.at[g], b_buf.at[g], b_send.at[d], b_recv.at[g], at(gs[d], s, e))
        a.start()
        sends.append(a)
    for d in (1, 3, 2):
        src = gs[d]
        arrived(b_buf.at[src], b_recv.at[src], b_send.at[0])
    hidden = ((b_buf[0] + b_buf[1]) + (b_buf[2] + b_buf[3])) + r16[...]
    c_buf[zc] = hidden.astype(BF16)
    for de in (4, 3, 5, 2, 6, 1, 7, 0):
        for dz in (1, 0):
            if de or dz:
                a = remote(
                    c_buf.at[zc], c_buf.at[zc], c_send.at[8 * dz + de], c_recv.at[zc],
                    at(g, peers[4 * dz], es[de]),
                )
                a.start()
                sends.append(a)
    for i in range(6, 9):
        loads[i].wait()

    for half in range(2):
        zz = zs[half]
        for d in range(half == 0, 8):
            src = zz * 8 + es[d]
            arrived(c_buf.at[src], c_recv.at[src], c_send.at[0])
        rows = c_buf[pl.ds(zz * 8, 8)].reshape(128, 128)
        taken = dot(select, rows).astype(BF16)
        for j in range(4):
            d_buf[y, zz, :, 128 * j : 128 * (j + 1)] = taken[16 * j : 16 * j + 16]
        for d in (2, 1, 3):
            a = remote(
                d_buf.at[y, zz], d_buf.at[y, zz], d_send.at[2 * d + half], d_recv.at[2 * y + zz],
                at(g, peers[d], e),
            )
            a.start()
            sends.append(a)

    square = jnp.zeros((16, 1), F32)
    logits = jnp.zeros((8, 16), F32)
    for n, d in enumerate((0, 1, 3, 2)):
        src = ys[d]
        gg, uu = jnp.zeros((448, 16), F32), jnp.zeros((448, 16), F32)
        for half in range(2):
            zz = zs[half]
            if d:
                arrived(d_buf.at[src, zz], d_recv.at[2 * src + zz], d_send.at[0])
            x = d_buf[src, zz].astype(F32)
            square = square + jnp.sum(x * x, axis=1, keepdims=True)
            block = zz * 4 + src
            cols = pl.ds(pl.multiple_of(block * 512, 512), 512)
            scales = gain_f[pl.ds(pl.multiple_of(block * 4, 4), 4), :]
            u = jnp.concatenate(
                [(x[:, 128 * j : 128 * (j + 1)] * scales[j : j + 1]).astype(BF16) for j in range(4)], axis=1
            )
            logits = logits + dot(rtr_v[:, cols], u, NT)
            gg, uu = gg + dot(wg_v[:, cols], u, NT), uu + dot(wu_v[:, cols], u, NT)
        if n == 0:
            gate_acc[...] = gg
            up_acc[...] = uu
        elif n < 3:
            gate_acc[...] += gg
            up_acc[...] += uu
    scale = to_row16(lax.rsqrt(square * (1.0 / 4096.0) + 1e-05))
    logits = logits * scale
    lrow = iota((8, 16), 0)
    own = jnp.sum(jnp.where(lrow == e, logits, 0.0), axis=0, keepdims=True)
    oth = jnp.sum(jnp.where(lrow.astype(F32) == other_row, logits, 0.0), axis=0, keepdims=True)
    share = 1.0 / (1.0 + jnp.exp(oth - own))
    gate = (gate_acc[...] + gg) * scale
    act = gate / (1.0 + jnp.exp(-gate)) * ((up_acc[...] + uu) * (scale * share))
    act = act.T.astype(BF16)
    loads[9].wait()

    for dy in (2, 1, 3, 0):
        ty = ys[dy]
        for zz in range(2):
            cols = pl.ds(pl.multiple_of((zz * 4 + ty) * 512, 512), 512)
            res = dot(act, wd_v[:, cols])
            for tx in range(4):
                tiles = []
                for j in range(2):
                    first = res[8 * (tx // 2) : 8 * (tx // 2) + 8, 256 * j : 256 * j + 128]
                    second = res[8 * (tx // 2) : 8 * (tx // 2) + 8, 256 * j + 128 : 256 * j + 256]
                    if tx % 2:
                        first = pltpu.roll(first, 4, 0)
                    else:
                        second = pltpu.roll(second, 4, 0)
                    tiles.append(jnp.where(low, first, second))
                e_src[tx * 4 + ty, 16 * zz : 16 * zz + 16, :] = jnp.concatenate(tiles, axis=0).astype(BF16)
        for dx in (2, 1, 3, 0):
            if dx or dy:
                t = gs[dx] * 4 + ty
                a = remote(
                    e_src.at[t], e_buf.at[xy], e_send.at[4 * dx + dy], e_recv.at[xy],
                    at(gs[dx], peers[dy], e),
                )
                a.start()
                sends.append(a)
    summed = e_src[xy].astype(F32)
    for dy in (0, 1, 3, 2):
        for dx in (0, 1, 3, 2):
            if dx or dy:
                src = gs[dx] * 4 + ys[dy]
                arrived(e_buf.at[src], e_recv.at[src], e_send.at[0])
                summed = summed + e_buf[src].astype(F32)
    for zz in range(2):
        g_src[zz] = summed[16 * zz : 16 * zz + 16].astype(BF16)
    later = []
    for zz in range(2):
        for tx in range(4):
            for cc in range(2):
                ee = g * 2 + cc
                same = (g == tx) & (zh == zz) & (e == ee)
                a = remote(
                    g_src.at[zz], g_buf.at[zc], g_send.at[zz * 8 + tx * 2 + cc], g_recv.at[zc],
                    at(tx, zz * 4 + y, ee),
                )
                pl.when(jnp.logical_not(same))(a.start)
                later.append((same, a))

    @pl.when(g == zl)
    def _():
        g_buf[zc] = g_src[zh]

    for t in range(16):
        @pl.when(jnp.logical_not((g == zl) & (zc == t)))
        def _(t=t):
            arrived(g_buf.at[t], g_recv.at[t], g_send.at[0])
    final = hidden + dot(comb, g_buf[...].reshape(256, 128))
    f16[...] = final
    for j in range(4):
        out_ref[:, 128 * j : 128 * (j + 1)] = f16[4 * j : 4 * j + 4, :].astype(BF16)

    for a in sends:
        a.wait_send()
    for same, a in later:
        pl.when(jnp.logical_not(same))(a.wait_send)


def shards(
    queries, keys, values, block_of_slot, lengths, out_proj, residual, norm_gain, router,
    routes, w_gate, w_up, w_down,
):
    args = (
        block_of_slot, lengths, routes.T,
        queries, keys.reshape(4, 256, 128), values.reshape(4, 256, 128), out_proj, residual,
        norm_gain.reshape(32, 128), router.T, w_gate[0].T, w_up[0].T, w_down[0],
    )
    hbm = pl.BlockSpec(memory_space=pltpu.HBM)
    dma = pltpu.SemaphoreType.DMA
    vmem = pltpu.VMEM
    return pl.pallas_call(
        kernel,
        out_shape=jax.ShapeDtypeStruct((4, 512), BF16),
        in_specs=[hbm] * 13,
        out_specs=pl.BlockSpec(memory_space=pltpu.VMEM),
        scratch_shapes=[pltpu.SMEM(a.shape, a.dtype) for a in args[:3]]
        + [vmem(a.shape, a.dtype) for a in args[3:]]
        + [
            vmem((8, 8, 128), I32),
            vmem((8, 32, 128), BF16), vmem((8, 2, 128), F32), vmem((32, 128), F32),
            vmem((64, 128), F32), vmem((16, 128), F32), vmem((4, 16, 128), F32),
            vmem((16, 16, 128), BF16), vmem((4, 2, 16, 512), BF16), vmem((16, 512), BF16),
            vmem((448, 16), F32), vmem((448, 16), F32),
            vmem((16, 32, 128), BF16), vmem((16, 32, 128), BF16),
            vmem((2, 16, 128), BF16), vmem((16, 16, 128), BF16), vmem((16, 128), F32),
            dma((10,)), dma((8,)), dma((8,)), dma((16,)), dma((16,)), dma((3,)),
            dma((4,)), dma((4,)), dma((16,)), dma((16,)), dma((8,)), dma((8,)),
            dma((16,)), dma((16,)), dma((16,)), dma((16,)),
        ],
        compiler_params=pltpu.CompilerParams(
            collective_id=0, has_side_effects=True, vmem_limit_bytes=67043328
        ),
    )(*args)


def solution(mesh):
    return jax.shard_map(
        shards,
        mesh=mesh,
        in_specs=(
            P("expert", "group", None),
            P("expert", "seq", "group", None),
            P("expert", "seq", "group", None),
            P("expert", "seq"),
            P("expert"),
            P("group", "seq"),
            P("expert", "seq"),
            P(),
            P(),
            P("expert", None),
            P("expert", None, ("group", "seq")),
            P("expert", None, ("group", "seq")),
            P("expert", ("group", "seq"), None),
        ),
        out_specs=P("expert", "seq"),
        check_vma=False,
    )
```

```python
import jax
import jax.numpy as jnp
from jax import lax
from jax.experimental import pallas as pl
from jax.experimental.pallas import tpu as pltpu
from jax.sharding import PartitionSpec as P

BLOCK = 16
MASKED = -1e30
F32 = jnp.float32
BF16 = jnp.bfloat16
I32 = jnp.int32
NT = (((1,), (1,)), ((), ()))
NN = (((1,), (0,)), ((), ()))


def dot(a, b, dims=NN):
    return lax.dot_general(a, b, dims, preferred_element_type=F32)


def iota(shape, dim):
    return lax.broadcasted_iota(I32, shape, dim)


def kernel(
    blk_h, len_h, rt_h,
    q_h, k_h, v_h, wo_h, res_h, gain_h, rtr_h, wg_h, wu_h, wd_h,
    out_ref,
    blk_s, len_s, rt_s,
    q_v, k_v, v_v, wo_v, res_v, gain_v, rtr_v, wg_v, wu_v, wd_v,
    rt_buf, o1, s1, gain_f, att, r16, b_buf, c_src, c_buf, d_buf, wgt, wut, gate_acc, up_acc,
    e_src, e_buf, g_src, g_buf, f16,
    local_sem, rt_send, rt_recv, a1_send, a1_recv, small_sem, b_send, b_recv,
    c_send, c_recv, d_send, d_recv, e_send, e_recv, g_send, g_recv,
):
    g = lax.axis_index("group")
    s = lax.axis_index("seq")
    e = lax.axis_index("expert")
    zh, y = lax.div(s, 4), lax.rem(s, 4)
    zl, core = lax.div(e, 2), lax.rem(e, 2)
    zc = zh * 8 + e
    xy = g * 4 + y
    oz = 1 - zh
    gs = [g] + [lax.rem(g + d, 4) for d in (1, 2, 3)]
    ys = [y] + [lax.rem(y + d, 4) for d in (1, 2, 3)]
    es = [e] + [lax.rem(e + d, 8) for d in range(1, 8)]
    zs = [zh, oz]
    peers = [zs[d // 4] * 4 + ys[d % 4] for d in range(8)]

    def at(gg, ss, ee):
        return {"group": gg, "seq": ss, "expert": ee}

    def remote(src, dst, ssem, rsem, where):
        return pltpu.make_async_remote_copy(
            src_ref=src, dst_ref=dst, send_sem=ssem, recv_sem=rsem,
            device_id=where, device_id_type=pl.DeviceIdType.MESH,
        )

    barrier = pltpu.get_barrier_semaphore()

    def greet(where):
        pl.semaphore_signal(barrier, inc=1, device_id=where, device_id_type=pl.DeviceIdType.MESH)

    for d in (6, 5, 7, 4, 2, 1, 3):
        greet(at(g, peers[d], e))
    for dz in (1, 0):
        for de in (4, 3, 5, 2, 6, 1, 7):
            greet(at(g, peers[4 * dz], es[de]))
    for d in (2, 1, 3):
        greet(at(gs[d], s, e))

    pairs = [
        (q_h, q_v), (k_h, k_v), (v_h, v_v), (wo_h, wo_v), (res_h, res_v),
        (gain_h, gain_v), (rtr_h, rtr_v), (wg_h, wg_v), (wu_h, wu_v), (wd_h, wd_v),
    ]
    loads = [pltpu.make_async_copy(a, b, local_sem.at[i]) for i, (a, b) in enumerate(pairs)]
    small = [
        pltpu.make_async_copy(a, b, small_sem.at[i])
        for i, (a, b) in enumerate([(rt_h, rt_s), (blk_h, blk_s), (len_h, len_s)])
    ]
    for load in loads[0:3] + small:
        load.start()

    for copy in small:
        copy.wait()
    row8, lane8 = iota((8, 128), 0), iota((8, 128), 1)
    codes = jnp.full((8, 128), -1, I32)
    count = jnp.zeros((8, 128), I32)
    for tok in range(4):
        first, second = rt_s[0, tok], rt_s[1, tok]
        hit0, hit1 = row8 == first, row8 == second
        hit = hit0 | hit1
        other = jnp.where(hit0, second, first)
        codes = jnp.where((lane8 % 4 == tok) & hit, count + 2 * other, codes)
        count = count + jnp.where(hit, 1, 0)
    rt_buf[e] = codes

    eye = iota((32, 128), 0) == iota((32, 128), 1)
    lane = iota((1, 256), 1)
    parity = iota((8, 256), 1) % 2 == iota((8, 256), 0) // 4
    for i in range(3):
        loads[i].wait()
    for load in loads[3:]:
        load.start()
    outs, maxes, sums = [], [], []
    for r in range(4):
        sc = dot(q_v[r], k_v[r], NT) * (128 ** -0.5)
        limit = jnp.zeros((1, 256), I32)
        for j in range(8):
            limit = jnp.where(lane // 32 == j, len_s[r] - BLOCK * blk_s[r, j], limit)
        live = parity & ((lane // 2) % BLOCK < limit)
        sc = jnp.where(live, sc, MASKED)
        m = jnp.max(sc, axis=1, keepdims=True)
        p = jnp.where(live, jnp.exp(sc - m), 0.0)
        sums.append(jnp.sum(p, axis=1, keepdims=True))
        maxes.append(m)
        outs.append(dot(p.astype(BF16), v_v[r]))

    def to_row(col):
        return jnp.sum(jnp.where(eye, col, 0.0), axis=0, keepdims=True)

    def to_col(row):
        return jnp.sum(jnp.where(eye, row, 0.0), axis=1, keepdims=True)

    o1[s] = jnp.concatenate(outs, axis=0).astype(BF16)
    s1[s, 0:1, :] = to_row(jnp.concatenate(maxes, axis=0))
    s1[s, 1:2, :] = to_row(jnp.concatenate(sums, axis=0))

    pl.semaphore_wait(barrier, 24)

    sends = []
    for d in (6, 5, 7, 4, 2, 1, 3):
        to = at(g, peers[d], e)
        a = remote(o1.at[s], o1.at[s], a1_send.at[2 * d], a1_recv.at[2 * s], to)
        b = remote(s1.at[s], s1.at[s], a1_send.at[2 * d + 1], a1_recv.at[2 * s + 1], to)
        a.start()
        b.start()
        sends += [a, b]
    for d in range(1, 8):
        to = at(g, s, es[d])
        a = remote(rt_buf.at[e], rt_buf.at[e], rt_send.at[d], rt_recv.at[e], to)
        a.start()
        sends.append(a)

    me = at(g, s, e)

    def arrived(dst, rsem, ssem):
        remote(dst, dst, ssem, rsem, me).wait_recv()

    loads[4].wait()
    for j in range(4):
        r16[4 * j : 4 * j + 4, :] = res_v[:, 128 * j : 128 * (j + 1)].astype(F32)
    clane = iota((16, 256), 1)
    crow = iota((16, 256), 0)
    comb = jnp.zeros((16, 256), F32)
    clane_e, clane_blk, clane_rank = (clane // 16) % 8, (clane // 4) % 4, clane % 2
    fits = ((clane // 2) % 2 == core) & (clane_blk == crow // 4)
    ccount = jnp.zeros((16, 256), I32)
    for tok in range(4):
        hit = (clane_e == rt_s[0, tok]) | (clane_e == rt_s[1, tok])
        comb = jnp.where(fits & hit & (crow % 4 == tok) & (ccount == clane_rank), 1.0, comb)
        ccount = ccount + jnp.where(hit, 1, 0)
    comb = comb.astype(BF16)
    prow, pcol = iota((64, 16), 0), iota((64, 16), 1)
    pfits = (prow // 2) % 4 == pcol // 4
    pack = jnp.zeros((64, 16), F32)
    pcount = jnp.zeros((64, 16), I32)
    for tok in range(4):
        hit = (prow // 8 == rt_s[0, tok]) | (prow // 8 == rt_s[1, tok])
        pack = jnp.where(pfits & hit & (pcol % 4 == tok) & (pcount == prow % 2), 1.0, pack)
        pcount = pcount + jnp.where(hit, 1, 0)
    pack = pack.astype(BF16)
    urow, ucol = iota((64, 64), 0), iota((64, 64), 1)
    unpack = jnp.where(
        (urow % 2 == ucol % 2) & ((urow // 2) % 8 == ucol // 8) & (urow // 16 == (ucol // 2) % 4),
        1.0, 0.0,
    ).astype(BF16)

    for d in range(1, 8):
        src = es[d]
        arrived(rt_buf.at[src], rt_recv.at[src], rt_send.at[0])
    lane1 = iota((1, 128), 1)
    code = jnp.full((1, 128), -1, I32)
    for i in range(8):
        mine = jnp.sum(jnp.where(row8 == e, rt_buf[i], 0), axis=0, keepdims=True)
        code = jnp.where(lane1 // 16 == i, mine, code)
    rank = jnp.where(code >= 0, code % 2, -1)
    other_lane = jnp.where(code >= 0, code // 2, 0)
    srow, slane = iota((16, 128), 0), iota((16, 128), 1)
    pick = (srow % 2 == rank) & (srow // 2 == slane // 16) & ((slane // 4) % 4 == 0)
    other_col = jnp.sum(
        jnp.where(pick, other_lane.astype(F32), 0.0), axis=1, keepdims=True
    )
    eye16 = iota((16, 128), 0) == iota((16, 128), 1)

    def to_row16(col):
        return jnp.sum(jnp.where(eye16, col, 0.0), axis=0, keepdims=True)[:, 0:16]

    other_row = to_row16(other_col)
    def turn(first, last):
        for n in range(first, last):
            src, dst = ((wg_v, wgt), (wu_v, wut))[n // 8]
            rows = pl.ds(512 * (n % 8), 512)
            dst[rows, :] = src[:, rows].T

    for i in (7, 8):
        loads[i].wait()
    turn(0, 9)
    loads[5].wait()
    gain_f[...] = gain_v[...].astype(F32)
    loads[3].wait()

    for d in (1, 3, 2, 4, 5, 7, 6):
        src = peers[d]
        arrived(o1.at[src], a1_recv.at[2 * src], a1_send.at[0])
        arrived(s1.at[src], a1_recv.at[2 * src + 1], a1_send.at[0])
    ms = [s1[i, 0:1, :] for i in range(8)]
    top = ms[0]
    for m in ms[1:]:
        top = jnp.maximum(top, m)
    ws = [jnp.exp(m - top) for m in ms]
    total = jnp.zeros((1, 128), F32)
    for i in range(8):
        total = total + ws[i] * s1[i, 1:2, :]
    merged = jnp.zeros((32, 128), F32)
    for i in range(8):
        merged = merged + to_col(ws[i] / total) * o1[i].astype(F32)
    att[0:32, :] = merged
    att[32:64, :] = merged
    part = jnp.zeros((8, 512), F32)
    for h in range(8):
        part = part + dot(att[pl.ds(h, 8, stride=8), :].astype(BF16), wo_v[128 * h : 128 * (h + 1), :])
    low = iota((8, 128), 0) < 4
    for j in range(2):
        b_buf[g, 8 * j : 8 * j + 8, :] = jnp.where(
            low, part[:, 256 * j : 256 * j + 128], part[:, 256 * j + 128 : 256 * j + 256]
        )
    for d in (2, 1, 3):
        a = remote(b_buf.at[g], b_buf.at[g], b_send.at[d], b_recv.at[g], at(gs[d], s, e))
        a.start()
        sends.append(a)
    for d in (1, 3, 2):
        src = gs[d]
        arrived(b_buf.at[src], b_recv.at[src], b_send.at[0])
    hidden = ((b_buf[0] + b_buf[1]) + (b_buf[2] + b_buf[3])) + r16[...]
    packed = dot(pack, hidden.astype(BF16)).astype(BF16)
    for i in range(8):
        c_src[i] = packed[8 * i : 8 * i + 8]
    c_buf[zc] = c_src[e]
    for de in (4, 3, 5, 2, 6, 1, 7, 0):
        for dz in (1, 0):
            if de or dz:
                a = remote(
                    c_src.at[es[de]], c_buf.at[zc], c_send.at[8 * dz + de], c_recv.at[zc],
                    at(g, peers[4 * dz], es[de]),
                )
                a.start()
                sends.append(a)
    loads[6].wait()
    turn(9, 16)

    for half in range(2):
        zz = zs[half]
        for d in range(half == 0, 8):
            src = zz * 8 + es[d]
            arrived(c_buf.at[src], c_recv.at[src], c_send.at[0])
        rows = c_buf[pl.ds(zz * 8, 8)].astype(F32).reshape(64, 128).astype(BF16)
        taken = dot(unpack, rows).astype(BF16)
        for j in range(4):
            d_buf[y, zz, :, 128 * j : 128 * (j + 1)] = taken[16 * j : 16 * j + 16]
        for d in (2, 1, 3):
            a = remote(
                d_buf.at[y, zz], d_buf.at[y, zz], d_send.at[2 * d + half], d_recv.at[2 * y + zz],
                at(g, peers[d], e),
            )
            a.start()
            sends.append(a)

    square = jnp.zeros((16, 1), F32)
    logits = jnp.zeros((8, 16), F32)
    for n, d in enumerate((0, 1, 3, 2)):
        src = ys[d]
        gg, uu = jnp.zeros((16, 448), F32), jnp.zeros((16, 448), F32)
        for half in range(2):
            zz = zs[half]
            if d:
                arrived(d_buf.at[src, zz], d_recv.at[2 * src + zz], d_send.at[0])
            x = d_buf[src, zz].astype(F32)
            square = square + jnp.sum(x * x, axis=1, keepdims=True)
            block = zz * 4 + src
            cols = pl.ds(pl.multiple_of(block * 512, 512), 512)
            scales = gain_f[pl.ds(pl.multiple_of(block * 4, 4), 4), :]
            u = jnp.concatenate(
                [(x[:, 128 * j : 128 * (j + 1)] * scales[j : j + 1]).astype(BF16) for j in range(4)], axis=1
            )
            logits = logits + dot(rtr_v[:, cols], u, NT)
            gg, uu = gg + dot(u, wgt[cols, :]), uu + dot(u, wut[cols, :])
        if n == 0:
            gate_acc[...] = gg
            up_acc[...] = uu
        elif n < 3:
            gate_acc[...] += gg
            up_acc[...] += uu
    scale = to_row16(lax.rsqrt(square * (1.0 / 4096.0) + 1e-05))
    factor = lax.rsqrt(square * (1.0 / 4096.0) + 1e-05)
    logits = logits * scale
    lrow = iota((8, 16), 0)
    own = jnp.sum(jnp.where(lrow == e, logits, 0.0), axis=0, keepdims=True)
    oth = jnp.sum(jnp.where(lrow.astype(F32) == other_row, logits, 0.0), axis=0, keepdims=True)
    share = 1.0 / (1.0 + jnp.exp(oth - own))
    share_col = jnp.sum(
        jnp.where(iota((16, 16), 0) == iota((16, 16), 1), share, 0.0), axis=1, keepdims=True
    )
    gate = (gate_acc[...] + gg) * factor
    act = gate / (1.0 + jnp.exp(-gate)) * ((up_acc[...] + uu) * (factor * share_col))
    act = act.astype(BF16)
    loads[9].wait()

    for dy in (2, 1, 3, 0):
        ty = ys[dy]
        for zz in range(2):
            cols = pl.ds(pl.multiple_of((zz * 4 + ty) * 512, 512), 512)
            res = dot(act, wd_v[:, cols])
            for tx in range(4):
                tiles = []
                for j in range(2):
                    first = res[8 * (tx // 2) : 8 * (tx // 2) + 8, 256 * j : 256 * j + 128]
                    second = res[8 * (tx // 2) : 8 * (tx // 2) + 8, 256 * j + 128 : 256 * j + 256]
                    if tx % 2:
                        first = pltpu.roll(first, 4, 0)
                    else:
                        second = pltpu.roll(second, 4, 0)
                    tiles.append(jnp.where(low, first, second))
                e_src[tx * 4 + ty, 16 * zz : 16 * zz + 16, :] = jnp.concatenate(tiles, axis=0).astype(BF16)
        for dx in (2, 1, 3, 0):
            if dx or dy:
                t = gs[dx] * 4 + ty
                a = remote(
                    e_src.at[t], e_buf.at[xy], e_send.at[4 * dx + dy], e_recv.at[xy],
                    at(gs[dx], peers[dy], e),
                )
                a.start()
                sends.append(a)
    summed = e_src[xy].astype(F32)
    for dy in (0, 1, 3, 2):
        for dx in (0, 1, 3, 2):
            if dx or dy:
                src = gs[dx] * 4 + ys[dy]
                arrived(e_buf.at[src], e_recv.at[src], e_send.at[0])
                summed = summed + e_buf[src].astype(F32)
    for zz in range(2):
        g_src[zz] = summed[16 * zz : 16 * zz + 16].astype(BF16)
    later = []
    for zz in range(2):
        for tx in range(4):
            for cc in range(2):
                ee = g * 2 + cc
                same = (g == tx) & (zh == zz) & (e == ee)
                a = remote(
                    g_src.at[zz], g_buf.at[zc], g_send.at[zz * 8 + tx * 2 + cc], g_recv.at[zc],
                    at(tx, zz * 4 + y, ee),
                )
                pl.when(jnp.logical_not(same))(a.start)
                later.append((same, a))

    @pl.when(g == zl)
    def _():
        g_buf[zc] = g_src[zh]

    for t in range(16):
        @pl.when(jnp.logical_not((g == zl) & (zc == t)))
        def _(t=t):
            arrived(g_buf.at[t], g_recv.at[t], g_send.at[0])
    final = hidden + dot(comb, g_buf[...].reshape(256, 128))
    f16[...] = final
    for j in range(4):
        out_ref[:, 128 * j : 128 * (j + 1)] = f16[4 * j : 4 * j + 4, :].astype(BF16)

    for a in sends:
        a.wait_send()
    for same, a in later:
        pl.when(jnp.logical_not(same))(a.wait_send)


def shards(
    queries, keys, values, block_of_slot, lengths, out_proj, residual, norm_gain, router,
    routes, w_gate, w_up, w_down,
):
    args = (
        block_of_slot, lengths, routes.T,
        queries, keys.reshape(4, 256, 128), values.reshape(4, 256, 128), out_proj, residual,
        norm_gain.reshape(32, 128), router.T, w_gate[0].T, w_up[0].T, w_down[0],
    )
    hbm = pl.BlockSpec(memory_space=pltpu.HBM)
    dma = pltpu.SemaphoreType.DMA
    vmem = pltpu.VMEM
    return pl.pallas_call(
        kernel,
        out_shape=jax.ShapeDtypeStruct((4, 512), BF16),
        in_specs=[hbm] * 13,
        out_specs=pl.BlockSpec(memory_space=pltpu.VMEM),
        scratch_shapes=[pltpu.SMEM(a.shape, a.dtype) for a in args[:3]]
        + [vmem(a.shape, a.dtype) for a in args[3:]]
        + [
            vmem((8, 8, 128), I32),
            vmem((8, 32, 128), BF16), vmem((8, 2, 128), F32), vmem((32, 128), F32),
            vmem((64, 128), F32), vmem((16, 128), F32), vmem((4, 16, 128), F32),
            vmem((8, 8, 128), BF16), vmem((16, 8, 128), BF16), vmem((4, 2, 16, 512), BF16), vmem((4096, 448), BF16), vmem((4096, 448), BF16),
            vmem((16, 448), F32), vmem((16, 448), F32),
            vmem((16, 32, 128), BF16), vmem((16, 32, 128), BF16),
            vmem((2, 16, 128), BF16), vmem((16, 16, 128), BF16), vmem((16, 128), F32),
            dma((10,)), dma((8,)), dma((8,)), dma((16,)), dma((16,)), dma((3,)),
            dma((4,)), dma((4,)), dma((16,)), dma((16,)), dma((8,)), dma((8,)),
            dma((16,)), dma((16,)), dma((16,)), dma((16,)),
        ],
        compiler_params=pltpu.CompilerParams(
            collective_id=0, has_side_effects=True, vmem_limit_bytes=67043328
        ),
    )(*args)


def solution(mesh):
    return jax.shard_map(
        shards,
        mesh=mesh,
        in_specs=(
            P("expert", "group", None),
            P("expert", "seq", "group", None),
            P("expert", "seq", "group", None),
            P("expert", "seq"),
            P("expert"),
            P("group", "seq"),
            P("expert", "seq"),
            P(),
            P(),
            P("expert", None),
            P("expert", None, ("group", "seq")),
            P("expert", None, ("group", "seq")),
            P("expert", ("group", "seq"), None),
        ),
        out_specs=P("expert", "seq"),
        check_vma=False,
    )
```
